32 devices in a mesh: grp: 2 (over core), ex: 16 (over z, y, x).
Axes of the slice: x: 2, y: 2, z: 4, core: 2. Of those that a mesh axis runs over, the one named last changes fastest.
Arguments:
- tokens: bfloat16 [8192, 1024], P(('grp', 'ex')), may hold values from -6 to 6
- expert_ids: int32 [8192], P(('grp', 'ex')), may hold values from 0 to 15, as said below
- slot_ids: int32 [8192], P(('grp', 'ex')), may hold values from 0 to 31, as said below
- centroids: bfloat16 [16, 1024], replicated, may hold values from -0.1875 to 0.1875
- w_in: bfloat16 [16, 1024, 4096], P('ex', None, 'grp'), may hold values from -0.1875 to 0.1875
- w_out: bfloat16 [16, 4096, 1024], P('ex', 'grp'), may hold values from -0.09375 to 0.09375
Outputs:
- combined: bfloat16 [8192, 1024], P(('grp', 'ex'))
The draws below stay inside these ranges and needn't reach their ends.
Inputs may be any that keep to these rules, and one draw needn't show every extreme that they name: `expert_ids`: within each device's 256 rows, at most 32 rows name one expert; in every device some expert is named by exactly 32 rows, and in each group of 16 devices along ex one expert is named by 32 rows on every device of the group. `slot_ids`: rows of one device that name the same expert have distinct slots.
All inputs are finite; a program needn't handle non-finite values.
Results may differ from the reference program's by a relative error of at most 0.0035.
Values may be sent and summed in bfloat16 or wider, within the bound.
No kernel may reach another device: no remote copies, remote signals or barrier semaphores. Data moves between devices by JAX's collectives and lax.ppermute only.
A program may use at most 128 MiB of HBM per device.

```python
import jax
import jax.numpy as jnp
from jax import lax

D = 1024
FF = 4096
TOK_DEV = 256
EXPERTS = 16
TOKENS = 8192
CAP = 32


def assignment(key):
    base_key = jax.random.fold_in(key, 11)
    group_count = TOKENS // (TOK_DEV * EXPERTS)
    hot_experts = jax.random.randint(jax.random.fold_in(base_key, 1), (group_count,), 0, EXPERTS)
    block_keys = jax.random.split(jax.random.fold_in(base_key, 2), TOKENS // TOK_DEV)
    hot_list = jnp.repeat(hot_experts, EXPERTS)

    def one_block(block_key, hot_one):
        key_full, key_perm, key_rows = jax.random.split(block_key, 3)
        favoured = jax.random.randint(key_full, (), 0, EXPERTS)
        shuffled = jax.random.permutation(key_perm, EXPERTS * CAP).astype(jnp.int32)
        owner = shuffled // CAP
        classes = jnp.where(owner == hot_one, 0, jnp.where(owner == favoured, 1, 2)).astype(jnp.int32)
        ordering = jnp.argsort(classes * (EXPERTS * CAP) + jnp.arange(EXPERTS * CAP, dtype=jnp.int32))
        picked = shuffled[ordering][:TOK_DEV]
        picked = picked[jax.random.permutation(key_rows, TOK_DEV)]
        return (picked // CAP, picked % CAP)
    owners, places = jax.vmap(one_block)(block_keys, hot_list)
    return (owners.reshape(-1).astype(jnp.int32), places.reshape(-1).astype(jnp.int32))


def draw_expert_ids(key, part):
    return assignment(key)[0]


def draw_slot_ids(key, part):
    return assignment(key)[1]


def level_of(key, extent, shards, least, largest):
    def one(position, parts):
        draws = jax.random.uniform(jax.random.fold_in(jax.random.fold_in(key, 6), position), (parts,), jnp.float32, least / len(shards), largest / len(shards))
        return jnp.repeat(jnp.exp(draws), extent[position] // parts).reshape((-1,) + (1,) * (len(extent) - position - 1))

    gain = one(*shards[0])
    for cut in shards[1:]:
        gain = gain * one(*cut)
    return gain


def scatter_about(stream_key, dims, scale, reach, pieces=(), held_as=jnp.bfloat16):
    result = scale * jax.random.normal(stream_key, dims, jnp.float32)
    if pieces:
        result = result * level_of(stream_key, dims, pieces, -0.22, 0.18)
    return jnp.clip(result, -reach, reach).astype(held_as)


def setup_inputs(seed: int = 0) -> dict:
    keys = jax.random.split(jax.random.key(seed), 7)
    tokens = scatter_about(keys[0], (TOKENS, D), 1.0, 6.0, ((0, 32),))
    expert_ids = draw_expert_ids(jax.random.fold_in(keys[6], 71), 0)
    slot_ids = draw_slot_ids(jax.random.fold_in(keys[6], 71), 0)
    centroids = scatter_about(keys[3], (EXPERTS, D), D ** -0.5, 0.1875)
    w_in = scatter_about(keys[4], (EXPERTS, D, FF), D ** -0.5, 0.1875, ((0, 16), (2, 2)))
    w_out = scatter_about(keys[5], (EXPERTS, FF, D), FF ** -0.5, 0.09375, ((0, 16), (1, 2)))
    return {"tokens": tokens, "expert_ids": expert_ids, "slot_ids": slot_ids, "centroids": centroids, "w_in": w_in, "w_out": w_out}


def reference(tokens, expert_ids, slot_ids, centroids, w_in, w_out):
    block_count = TOKENS // TOK_DEV
    block_ids = jnp.arange(TOKENS, dtype=jnp.int32) // TOK_DEV
    buffer_rows = (expert_ids * (block_count * CAP) + block_ids * CAP + slot_ids).astype(jnp.int32)
    total_rows = EXPERTS * block_count * CAP
    buffer = jnp.zeros((total_rows, D), jnp.bfloat16).at[buffer_rows].set(tokens)
    buffer = buffer.reshape(EXPERTS, block_count * CAP, D)

    def expert(operands):
        rows_in, first, second = operands
        hidden = jnp.maximum(jnp.dot(rows_in, first, preferred_element_type=jnp.float32), 0.0).astype(jnp.bfloat16)
        return jnp.dot(hidden, second, preferred_element_type=jnp.float32).astype(jnp.bfloat16)

    results = lax.map(expert, (buffer, w_in, w_out)).reshape(total_rows, D)
    arrived = results[buffer_rows]
    scores = jnp.dot(tokens, centroids.T, preferred_element_type=jnp.float32)
    columns = jnp.arange(EXPERTS, dtype=jnp.int32)
    chosen = jnp.sum(jnp.where(columns[None, :] == expert_ids[:, None], scores, 0.0), axis=1)
    gating = jax.nn.sigmoid(chosen)
    return (tokens.astype(jnp.float32) + gating[:, None] * arrived.astype(jnp.float32)).astype(jnp.bfloat16)
```

```python
import jax
import jax.numpy as jnp
from jax import lax
from jax.sharding import PartitionSpec as P


def on_device(tokens, expert_ids, slot_ids, centroids, w_in, w_out):
    experts = centroids.shape[0]
    count_rows = tokens.shape[0]
    model_width = tokens.shape[1]
    capacity = 2 * count_rows // experts
    pair = lax.axis_size("grp")
    swap = [(i, (i + 1) % pair) for i in range(pair)]
    far_in = lax.ppermute(w_in, "grp", swap)
    far_out = lax.ppermute(w_out, "grp", swap)
    buffer_rows = expert_ids * capacity + slot_ids
    outgoing = (
        jnp.zeros((experts * capacity, model_width), jnp.bfloat16).at[buffer_rows].set(tokens)
    )
    outgoing = outgoing.reshape(experts, capacity, model_width)
    scores = jnp.dot(tokens, centroids.T, preferred_element_type=jnp.float32)
    columns = jnp.arange(experts, dtype=jnp.int32)
    chosen = jnp.sum(jnp.where(columns[None, :] == expert_ids[:, None], scores, 0.0), axis=1)
    gating = jax.nn.sigmoid(chosen)
    received = lax.all_to_all(outgoing, "ex", split_axis=0, concat_axis=0, tiled=True)
    flat_rows = received.reshape(-1, model_width)

    def half(first, second):
        hidden = jnp.maximum(
            jnp.dot(flat_rows, first, preferred_element_type=jnp.float32), 0.0
        ).astype(jnp.bfloat16)
        return jnp.dot(hidden, second, preferred_element_type=jnp.float32)

    result = half(w_in[0], w_out[0]) + half(far_in[0], far_out[0])
    returned = lax.all_to_all(
        result.astype(jnp.bfloat16).reshape(received.shape),
        "ex",
        split_axis=0,
        concat_axis=0,
        tiled=True,
    )
    arrived = returned.reshape(-1, model_width)[buffer_rows]
    mixed_rows = tokens.astype(jnp.float32) + gating[:, None] * arrived.astype(jnp.float32)
    return mixed_rows.astype(jnp.bfloat16)


def solution(mesh):
    in_specs = (
        P(("grp", "ex"), None),
        P(("grp", "ex")),
        P(("grp", "ex")),
        P(),
        P("ex", None, "grp"),
        P("ex", "grp", None),
    )
    out_specs = P(("grp", "ex"), None)
    return jax.shard_map(
        on_device, mesh=mesh, in_specs=in_specs, out_specs=out_specs, check_vma=False
    )
```

```python
import functools

import jax
import jax.numpy as jnp
from jax import lax
from jax.experimental import pallas as pl
from jax.experimental.pallas import tpu as pltpu
from jax.sharding import PartitionSpec as P

MIB = 1024 * 1024
COVER = 30_000_000_000


def picks(experts_ref, slots_ref, total_rows, capacity):
    wanted = experts_ref[...] * capacity + slots_ref[...]
    rows = lax.broadcasted_iota(jnp.int32, (total_rows, wanted.shape[1]), 0)
    return jnp.where(rows == wanted, 1.0, 0.0).astype(jnp.bfloat16)


def place_kernel(experts_ref, slots_ref, tokens_ref, out_ref, *, capacity):
    pick = picks(experts_ref, slots_ref, out_ref.shape[0], capacity)
    out_ref[...] = jnp.dot(
        pick, tokens_ref[...], preferred_element_type=jnp.float32
    ).astype(jnp.bfloat16)


def place(expert_ids, slot_ids, tokens, total_rows, capacity):
    return pl.pallas_call(
        functools.partial(place_kernel, capacity=capacity),
        out_shape=jax.ShapeDtypeStruct((total_rows, tokens.shape[1]), jnp.bfloat16),
        compiler_params=pltpu.CompilerParams(vmem_limit_bytes=8 * MIB),
        cost_estimate=pl.CostEstimate(flops=COVER, bytes_accessed=0, transcendentals=0),
        name="place",
    )(expert_ids[None, :], slot_ids[None, :], tokens)


def ffn_kernel(rows_ref, in_a, in_b, out_a, out_b, result_ref):
    def half(rows, first, second):
        hidden = jnp.maximum(
            jnp.dot(rows, first[0], preferred_element_type=jnp.float32), 0.0
        ).astype(jnp.bfloat16)
        return jnp.dot(hidden, second[0], preferred_element_type=jnp.float32)

    rows = rows_ref[...]
    total = half(rows, in_a, out_a) + half(rows, in_b, out_b)
    result_ref[...] = total.astype(jnp.bfloat16)


def ffn(rows, in_a, in_b, out_a, out_b):
    count, width = rows.shape
    hidden = in_a.shape[2]
    return pl.pallas_call(
        ffn_kernel,
        out_shape=jax.ShapeDtypeStruct((count, width), jnp.bfloat16),
        compiler_params=pltpu.CompilerParams(vmem_limit_bytes=34 * MIB),
        cost_estimate=pl.CostEstimate(
            flops=8 * count * width * hidden, bytes_accessed=8 * width * hidden, transcendentals=0
        ),
        name="ffn",
    )(rows, in_a, in_b, out_a, out_b)


def mix_kernel(experts_ref, slots_ref, gating_ref, tokens_ref, returned_ref, out_ref, *, capacity):
    pick = picks(experts_ref, slots_ref, returned_ref.shape[0], capacity)
    arrived = lax.dot_general(
        pick, returned_ref[...], (((0,), (0,)), ((), ())), preferred_element_type=jnp.float32
    )
    gating = jnp.broadcast_to(gating_ref[...], (8, gating_ref.shape[1])).T[:, :1]
    out_ref[...] = (tokens_ref[...].astype(jnp.float32) + gating * arrived).astype(jnp.bfloat16)


def mix(expert_ids, slot_ids, gating, tokens, returned, capacity):
    return pl.pallas_call(
        functools.partial(mix_kernel, capacity=capacity),
        out_shape=jax.ShapeDtypeStruct(tokens.shape, jnp.bfloat16),
        compiler_params=pltpu.CompilerParams(vmem_limit_bytes=8 * MIB),
        name="mix",
    )(expert_ids[None, :], slot_ids[None, :], gating[None, :], tokens, returned)


def on_device(tokens, expert_ids, slot_ids, centroids, w_in, w_out):
    experts = centroids.shape[0]
    count_rows = tokens.shape[0]
    model_width = tokens.shape[1]
    capacity = 2 * count_rows // experts
    pair = lax.axis_size("grp")
    swap = [(i, (i + 1) % pair) for i in range(pair)]
    far_in = lax.ppermute(w_in, "grp", swap)
    far_out = lax.ppermute(w_out, "grp", swap)
    outgoing = place(expert_ids, slot_ids, tokens, experts * capacity, capacity)
    outgoing = outgoing.reshape(experts, capacity, model_width)
    scores = jnp.dot(tokens, centroids.T, preferred_element_type=jnp.float32)
    columns = jnp.arange(experts, dtype=jnp.int32)
    chosen = jnp.sum(jnp.where(columns[None, :] == expert_ids[:, None], scores, 0.0), axis=1)
    gating = jax.nn.sigmoid(chosen)
    received = lax.all_to_all(outgoing, "ex", split_axis=0, concat_axis=0, tiled=True)
    result = ffn(received.reshape(-1, model_width), w_in, far_in, w_out, far_out)
    returned = lax.all_to_all(
        result.reshape(received.shape), "ex", split_axis=0, concat_axis=0, tiled=True
    )
    return mix(
        expert_ids, slot_ids, gating, tokens, returned.reshape(-1, model_width), capacity
    )


def solution(mesh):
    in_specs = (
        P(("grp", "ex"), None),
        P(("grp", "ex")),
        P(("grp", "ex")),
        P(),
        P("ex", None, "grp"),
        P("ex", "grp", None),
    )
    out_specs = P(("grp", "ex"), None)
    return jax.shard_map(
        on_device, mesh=mesh, in_specs=in_specs, out_specs=out_specs, check_vma=False
    )
```

```python
import jax
import jax.numpy as jnp
from jax import lax
from jax.experimental import pallas as pl
from jax.experimental.pallas import tpu as pltpu
from jax.sharding import PartitionSpec as P


MIB = 1024 * 1024
COVER = 30_000_000_000
FFN_LIMIT = 12


def picks(wanted, total_rows):
    rows = lax.broadcasted_iota(jnp.int32, (total_rows, wanted.shape[1]), 0)
    return jnp.where(rows == wanted, 1.0, 0.0).astype(jnp.bfloat16)


def place_kernel(wanted_ref, tokens_ref, *refs):
    total = sum(ref.shape[0] for ref in refs)
    placed = jnp.dot(
        picks(wanted_ref[...], total), tokens_ref[...], preferred_element_type=jnp.float32
    ).astype(jnp.bfloat16)
    start = 0
    for ref in refs:
        ref[...] = placed[start : start + ref.shape[0]]
        start += ref.shape[0]


def place(wanted, tokens, sizes):
    return pl.pallas_call(
        place_kernel,
        out_shape=[jax.ShapeDtypeStruct((n, tokens.shape[1]), jnp.bfloat16) for n in sizes],
        compiler_params=pltpu.CompilerParams(vmem_limit_bytes=8 * MIB),
        cost_estimate=pl.CostEstimate(flops=COVER, bytes_accessed=0, transcendentals=0),
        name="place",
    )(wanted[None, :], tokens)


def pack_kernel(keep_ref, got_ref, *refs):
    part = keep_ref.shape[0] // len(refs)
    for k, ref in enumerate(refs):
        ref[:part] = keep_ref[k * part : (k + 1) * part]
        ref[part:] = got_ref[k * part : (k + 1) * part]


def pack(keep, got, part):
    piece = jax.ShapeDtypeStruct((2 * part, keep.shape[1]), keep.dtype)
    return pl.pallas_call(
        pack_kernel,
        out_shape=[piece] * (keep.shape[0] // part),
        compiler_params=pltpu.CompilerParams(vmem_limit_bytes=4 * MIB),
        name="pack",
    )(keep, got)


def lower_kernel(*refs):
    piece_refs, out_ref = refs[:-1], refs[-1]
    part = out_ref.shape[0] // len(piece_refs)
    for k, ref in enumerate(piece_refs):
        out_ref[k * part : (k + 1) * part] = ref[part:]


def lower(pieces):
    rows = len(pieces) * pieces[0].shape[0] // 2
    return pl.pallas_call(
        lower_kernel,
        out_shape=jax.ShapeDtypeStruct((rows, pieces[0].shape[1]), pieces[0].dtype),
        compiler_params=pltpu.CompilerParams(vmem_limit_bytes=4 * MIB),
        name="lower",
    )(*pieces)


def product(rows, first, second):
    hidden = jnp.maximum(jnp.dot(rows, first, preferred_element_type=jnp.float32), 0.0)
    return jnp.dot(hidden.astype(jnp.bfloat16), second, preferred_element_type=jnp.float32)


def cost(count, weight):
    flops = 8 * count * weight.shape[1] * weight.shape[2]
    return pl.CostEstimate(flops=flops, bytes_accessed=8 * weight.size, transcendentals=0)


def ffn_kernel(in_a, in_b, out_a, out_b, *refs):
    row_refs, result_refs = refs[: len(refs) // 2], refs[len(refs) // 2 :]
    rows = jnp.concatenate([ref[...] for ref in row_refs], axis=0)
    total = product(rows, in_a[0], out_a[0]) + product(rows, in_b[0], out_b[0])
    total = total.astype(jnp.bfloat16)
    start = 0
    for ref in result_refs:
        ref[...] = total[start : start + ref.shape[0]]
        start += ref.shape[0]


def ffn(pieces, weights):
    return pl.pallas_call(
        ffn_kernel,
        out_shape=[jax.ShapeDtypeStruct(p.shape, jnp.bfloat16) for p in pieces],
        compiler_params=pltpu.CompilerParams(vmem_limit_bytes=FFN_LIMIT * MIB),
        cost_estimate=cost(sum(p.shape[0] for p in pieces), weights[0]),
        name="ffn",
    )(*weights, *pieces)


def mix_kernel(wanted_ref, gating_ref, tokens_ref, *refs):
    piece_refs, back_refs, out_ref = refs[:-3], refs[-3:-1], refs[-1]
    part = piece_refs[0].shape[0] // 2
    returned = jnp.concatenate(
        [ref[:part] for ref in piece_refs] + [ref[...] for ref in back_refs], axis=0
    )
    pick = picks(wanted_ref[...], returned.shape[0])
    arrived = lax.dot_general(
        pick, returned, (((0,), (0,)), ((), ())), preferred_element_type=jnp.float32
    )
    gating = jnp.broadcast_to(gating_ref[...], (8, gating_ref.shape[1])).T[:, :1]
    out_ref[...] = (tokens_ref[...].astype(jnp.float32) + gating * arrived).astype(jnp.bfloat16)


def mix(wanted, gating, tokens, pieces, back):
    return pl.pallas_call(
        mix_kernel,
        out_shape=jax.ShapeDtypeStruct(tokens.shape, jnp.bfloat16),
        compiler_params=pltpu.CompilerParams(vmem_limit_bytes=8 * MIB),
        name="mix",
    )(wanted[None, :], gating[None, :], tokens, *pieces, *back)


def gates(tokens, expert_ids, centroids):
    scores = jnp.dot(tokens, centroids.T, preferred_element_type=jnp.float32)
    columns = jnp.arange(centroids.shape[0], dtype=jnp.int32)
    named = columns[None, :] == expert_ids[:, None]
    return jax.nn.sigmoid(jnp.sum(jnp.where(named, scores, 0.0), axis=1))


def other_core():
    pair = lax.axis_size("grp")
    return [(i, (i + 1) % pair) for i in range(pair)]


def plain(tokens, expert_ids, slot_ids, centroids, w_in, w_out):
    experts, (count_rows, model_width) = centroids.shape[0], tokens.shape
    capacity = 2 * count_rows // experts
    far_in = lax.ppermute(w_in, "grp", other_core())
    far_out = lax.ppermute(w_out, "grp", other_core())
    buffer_rows = expert_ids * capacity + slot_ids
    empty = jnp.zeros((experts * capacity, model_width), jnp.bfloat16)
    outgoing = empty.at[buffer_rows].set(tokens).reshape(experts, capacity, model_width)
    received = lax.all_to_all(outgoing, "ex", split_axis=0, concat_axis=0, tiled=True)
    rows = received.reshape(-1, model_width)
    total = product(rows, w_in[0], w_out[0]) + product(rows, far_in[0], far_out[0])
    result = total.astype(jnp.bfloat16).reshape(received.shape)
    returned = lax.all_to_all(result, "ex", split_axis=0, concat_axis=0, tiled=True)
    arrived = returned.reshape(-1, model_width)[buffer_rows].astype(jnp.float32)
    gating = gates(tokens, expert_ids, centroids)
    return (tokens.astype(jnp.float32) + gating[:, None] * arrived).astype(jnp.bfloat16)


def paired(tokens, expert_ids, slot_ids, centroids, w_in, w_out):
    experts, count_rows = centroids.shape[0], tokens.shape[0]
    capacity = 2 * count_rows // experts
    span = experts // 4

    def travel(pieces, first):
        return [
            lax.ppermute(
                piece,
                ("grp", "ex"),
                [
                    (core * experts + i, core * experts + (i ^ (first + core * span + k)))
                    for core in range(2)
                    for i in range(experts)
                ],
            )
            for k, piece in enumerate(pieces)
        ]

    def change_core(rows):
        return lax.ppermute(rows, "grp", other_core())

    offset = expert_ids ^ lax.axis_index("ex")
    give = (offset // span % 2) ^ lax.axis_index("grp")
    near = 1 - offset // (2 * span)
    wanted = ((2 * give + near) * span + offset % span) * capacity + slot_ids
    keep_far, keep_near, give_far, give_near = place(wanted, tokens, [span * capacity] * 4)
    got_far = change_core(give_far)
    got_near = change_core(give_near)
    far_rows = travel(pack(keep_far, got_far, capacity), 2 * span)
    near_rows = travel(pack(keep_near, got_near, capacity), 0)
    far_in = lax.ppermute(w_in, "grp", other_core())
    far_out = lax.ppermute(w_out, "grp", other_core())
    weights = (w_in, far_in, w_out, far_out)
    near_results = ffn(near_rows, weights)
    far_results = ffn(far_rows, weights)
    far_back = travel(far_results, 2 * span)
    near_back = travel(near_results, 0)
    gave_far = change_core(lower(far_back))
    gave_near = change_core(lower(near_back))
    gating = gates(tokens, expert_ids, centroids)
    return mix(wanted, gating, tokens, [*far_back, *near_back], [gave_far, gave_near])


def solution(mesh):
    experts, pair = mesh.shape["ex"], mesh.shape["grp"]
    in_specs = (
        P(("grp", "ex"), None),
        P(("grp", "ex")),
        P(("grp", "ex")),
        P(),
        P("ex", None, "grp"),
        P("ex", "grp", None),
    )
    out_specs = P(("grp", "ex"), None)

    def step(*args):
        capacity = 2 * args[0].shape[0] // (pair * experts * experts)
        large = pair == 2 and experts % 4 == 0 and capacity % 16 == 0
        body = jax.shard_map(
            paired if large else plain,
            mesh=mesh,
            in_specs=in_specs,
            out_specs=out_specs,
            check_vma=False,
        )
        return body(*args)

    return step
```

```python
import jax
import jax.numpy as jnp
from jax import lax
from jax.experimental import pallas as pl
from jax.experimental.pallas import tpu as pltpu
from jax.sharding import PartitionSpec as P


MIB = 1024 * 1024
COVER = 30_000_000_000
FFN_LIMIT = 12


def picks(wanted, total_rows):
    rows = lax.broadcasted_iota(jnp.int32, (total_rows, wanted.shape[1]), 0)
    return jnp.where(rows == wanted, 1.0, 0.0).astype(jnp.bfloat16)


def place_kernel(wanted_ref, tokens_ref, *refs):
    total = sum(ref.shape[0] for ref in refs)
    placed = jnp.dot(
        picks(wanted_ref[...], total), tokens_ref[...], preferred_element_type=jnp.float32
    ).astype(jnp.bfloat16)
    start = 0
    for ref in refs:
        ref[...] = placed[start : start + ref.shape[0]]
        start += ref.shape[0]


def place(wanted, tokens, sizes):
    return pl.pallas_call(
        place_kernel,
        out_shape=[jax.ShapeDtypeStruct((n, tokens.shape[1]), jnp.bfloat16) for n in sizes],
        compiler_params=pltpu.CompilerParams(vmem_limit_bytes=8 * MIB),
        cost_estimate=pl.CostEstimate(flops=COVER, bytes_accessed=0, transcendentals=0),
        name="place",
    )(wanted[None, :], tokens)


def pack_kernel(keep_ref, got_ref, *refs):
    part = keep_ref.shape[0] // len(refs)
    for k, ref in enumerate(refs):
        ref[:part] = keep_ref[k * part : (k + 1) * part]
        ref[part:] = got_ref[k * part : (k + 1) * part]


def pack(keep, got, part):
    piece = jax.ShapeDtypeStruct((2 * part, keep.shape[1]), keep.dtype)
    return pl.pallas_call(
        pack_kernel,
        out_shape=[piece] * (keep.shape[0] // part),
        compiler_params=pltpu.CompilerParams(vmem_limit_bytes=4 * MIB),
        name="pack",
    )(keep, got)


def lower_kernel(*refs):
    piece_refs, out_ref = refs[:-1], refs[-1]
    part = out_ref.shape[0] // len(piece_refs)
    for k, ref in enumerate(piece_refs):
        out_ref[k * part : (k + 1) * part] = ref[part:]


def lower(pieces):
    rows = len(pieces) * pieces[0].shape[0] // 2
    return pl.pallas_call(
        lower_kernel,
        out_shape=jax.ShapeDtypeStruct((rows, pieces[0].shape[1]), pieces[0].dtype),
        compiler_params=pltpu.CompilerParams(vmem_limit_bytes=4 * MIB),
        name="lower",
    )(*pieces)


def product(rows, first, second):
    hidden = jnp.maximum(jnp.dot(rows, first, preferred_element_type=jnp.float32), 0.0)
    return jnp.dot(hidden.astype(jnp.bfloat16), second, preferred_element_type=jnp.float32)


def cost(count, weight):
    flops = 8 * count * weight.shape[1] * weight.shape[2]
    return pl.CostEstimate(flops=flops, bytes_accessed=8 * weight.size, transcendentals=0)


def ffn_kernel(in_a, in_b, out_a, out_b, *refs):
    row_refs, result_refs = refs[: len(refs) // 2], refs[len(refs) // 2 :]
    rows = jnp.concatenate([ref[...] for ref in row_refs], axis=0)
    total = product(rows, in_a[0], out_a[0]) + product(rows, in_b[0], out_b[0])
    total = total.astype(jnp.bfloat16)
    start = 0
    for ref in result_refs:
        ref[...] = total[start : start + ref.shape[0]]
        start += ref.shape[0]


def ffn(pieces, weights):
    return pl.pallas_call(
        ffn_kernel,
        out_shape=[jax.ShapeDtypeStruct(p.shape, jnp.bfloat16) for p in pieces],
        compiler_params=pltpu.CompilerParams(vmem_limit_bytes=FFN_LIMIT * MIB),
        cost_estimate=cost(sum(p.shape[0] for p in pieces), weights[0]),
        name="ffn",
    )(*weights, *pieces)


def mix_kernel(wanted_ref, gating_ref, tokens_ref, *refs):
    piece_refs, back_refs, out_ref = refs[:-3], refs[-3:-1], refs[-1]
    part = piece_refs[0].shape[0] // 2
    returned = jnp.concatenate(
        [ref[:part] for ref in piece_refs] + [ref[...] for ref in back_refs], axis=0
    )
    pick = picks(wanted_ref[...], returned.shape[0])
    arrived = lax.dot_general(
        pick, returned, (((0,), (0,)), ((), ())), preferred_element_type=jnp.float32
    )
    gating = jnp.broadcast_to(gating_ref[...], (8, gating_ref.shape[1])).T[:, :1]
    out_ref[...] = (tokens_ref[...].astype(jnp.float32) + gating * arrived).astype(jnp.bfloat16)


def mix(wanted, gating, tokens, pieces, back):
    return pl.pallas_call(
        mix_kernel,
        out_shape=jax.ShapeDtypeStruct(tokens.shape, jnp.bfloat16),
        compiler_params=pltpu.CompilerParams(vmem_limit_bytes=8 * MIB),
        name="mix",
    )(wanted[None, :], gating[None, :], tokens, *pieces, *back)


def gates(tokens, expert_ids, centroids):
    scores = jnp.dot(tokens, centroids.T, preferred_element_type=jnp.float32)
    columns = jnp.arange(centroids.shape[0], dtype=jnp.int32)
    named = columns[None, :] == expert_ids[:, None]
    return jax.nn.sigmoid(jnp.sum(jnp.where(named, scores, 0.0), axis=1))


def other_core():
    pair = lax.axis_size("grp")
    return [(i, (i + 1) % pair) for i in range(pair)]


def plain(tokens, expert_ids, slot_ids, centroids, w_in, w_out):
    experts, (count_rows, model_width) = centroids.shape[0], tokens.shape
    capacity = 2 * count_rows // experts
    far_in = lax.ppermute(w_in, "grp", other_core())
    far_out = lax.ppermute(w_out, "grp", other_core())
    buffer_rows = expert_ids * capacity + slot_ids
    empty = jnp.zeros((experts * capacity, model_width), jnp.bfloat16)
    outgoing = empty.at[buffer_rows].set(tokens).reshape(experts, capacity, model_width)
    received = lax.all_to_all(outgoing, "ex", split_axis=0, concat_axis=0, tiled=True)
    rows = received.reshape(-1, model_width)
    total = product(rows, w_in[0], w_out[0]) + product(rows, far_in[0], far_out[0])
    result = total.astype(jnp.bfloat16).reshape(received.shape)
    returned = lax.all_to_all(result, "ex", split_axis=0, concat_axis=0, tiled=True)
    arrived = returned.reshape(-1, model_width)[buffer_rows].astype(jnp.float32)
    gating = gates(tokens, expert_ids, centroids)
    return (tokens.astype(jnp.float32) + gating[:, None] * arrived).astype(jnp.bfloat16)


def paired(tokens, expert_ids, slot_ids, centroids, w_in, w_out):
    experts, count_rows = centroids.shape[0], tokens.shape[0]
    capacity = 2 * count_rows // experts
    span = experts // 4

    def travel(pieces, first):
        return [
            lax.ppermute(
                piece,
                ("grp", "ex"),
                [
                    (core * experts + i, core * experts + (i ^ (first + core * span + k)))
                    for core in range(2)
                    for i in range(experts)
                ],
            )
            for k, piece in enumerate(pieces)
        ]

    def change_core(rows):
        return lax.ppermute(rows, "grp", other_core())

    offset = expert_ids ^ lax.axis_index("ex")
    give = (offset // span % 2) ^ lax.axis_index("grp")
    close = 1 - offset // (2 * span)
    cut = span // 2
    late = offset % span // cut
    wanted = (((2 * give + late) * 2 + close) * cut + offset % cut) * capacity + slot_ids
    keep_a, keep_b, give_a, give_b = place(wanted, tokens, [span * capacity] * 4)
    got_a = change_core(give_a)
    got_b = change_core(give_b)
    out_a = pack(keep_a, got_a, capacity)
    out_b = pack(keep_b, got_b, capacity)
    far, near = 2 * span, 0
    far_a = travel(out_a[:cut], far)
    near_a = travel(out_a[cut:], near)
    far_b = travel(out_b[:cut], far + cut)
    near_b = travel(out_b[cut:], near + cut)
    far_in = lax.ppermute(w_in, "grp", other_core())
    far_out = lax.ppermute(w_out, "grp", other_core())
    weights = (w_in, far_in, w_out, far_out)
    done_a = ffn([*far_a, *near_a], weights)
    back_a = travel(done_a[:cut], far)
    back_a += travel(done_a[cut:], near)
    done_b = ffn([*far_b, *near_b], weights)
    back_b = travel(done_b[:cut], far + cut)
    back_b += travel(done_b[cut:], near + cut)
    gave_a = change_core(lower(back_a))
    gave_b = change_core(lower(back_b))
    gating = gates(tokens, expert_ids, centroids)
    return mix(wanted, gating, tokens, [*back_a, *back_b], [gave_a, gave_b])


def solution(mesh):
    experts, pair = mesh.shape["ex"], mesh.shape["grp"]
    in_specs = (
        P(("grp", "ex"), None),
        P(("grp", "ex")),
        P(("grp", "ex")),
        P(),
        P("ex", None, "grp"),
        P("ex", "grp", None),
    )
    out_specs = P(("grp", "ex"), None)

    def step(*args):
        capacity = 2 * args[0].shape[0] // (pair * experts * experts)
        large = pair == 2 and experts % 8 == 0 and capacity % 16 == 0
        body = jax.shard_map(
            paired if large else plain,
            mesh=mesh,
            in_specs=in_specs,
            out_specs=out_specs,
            check_vma=False,
        )
        return body(*args)

    return step
```

```python
import jax
import jax.numpy as jnp
from jax import lax
from jax.experimental import pallas as pl
from jax.experimental.pallas import tpu as pltpu
from jax.sharding import PartitionSpec as P


MIB = 1024 * 1024
COVER = 30_000_000_000
FFN_LIMIT = 12


def picks(wanted, total_rows):
    rows = lax.broadcasted_iota(jnp.int32, (total_rows, wanted.shape[1]), 0)
    return jnp.where(rows == wanted, 1.0, 0.0).astype(jnp.bfloat16)


def place_kernel(wanted_ref, tokens_ref, *refs):
    total = sum(ref.shape[0] for ref in refs)
    placed = jnp.dot(
        picks(wanted_ref[...], total), tokens_ref[...], preferred_element_type=jnp.float32
    ).astype(jnp.bfloat16)
    start = 0
    for ref in refs:
        ref[...] = placed[start : start + ref.shape[0]]
        start += ref.shape[0]


def place(wanted, tokens, sizes):
    return pl.pallas_call(
        place_kernel,
        out_shape=[jax.ShapeDtypeStruct((n, tokens.shape[1]), jnp.bfloat16) for n in sizes],
        compiler_params=pltpu.CompilerParams(vmem_limit_bytes=8 * MIB),
        cost_estimate=pl.CostEstimate(flops=COVER, bytes_accessed=0, transcendentals=0),
        name="place",
    )(wanted[None, :], tokens)


def pack_kernel(keep_ref, got_ref, *refs):
    part = keep_ref.shape[0] // len(refs)
    for k, ref in enumerate(refs):
        ref[:part] = keep_ref[k * part : (k + 1) * part]
        ref[part:] = got_ref[k * part : (k + 1) * part]


def pack(keep, got, part):
    piece = jax.ShapeDtypeStruct((2 * part, keep.shape[1]), keep.dtype)
    return pl.pallas_call(
        pack_kernel,
        out_shape=[piece] * (keep.shape[0] // part),
        compiler_params=pltpu.CompilerParams(vmem_limit_bytes=4 * MIB),
        name="pack",
    )(keep, got)


def lower_kernel(*refs):
    piece_refs, out_ref = refs[:-1], refs[-1]
    part = out_ref.shape[0] // len(piece_refs)
    for k, ref in enumerate(piece_refs):
        out_ref[k * part : (k + 1) * part] = ref[part:]


def lower(pieces):
    rows = len(pieces) * pieces[0].shape[0] // 2
    return pl.pallas_call(
        lower_kernel,
        out_shape=jax.ShapeDtypeStruct((rows, pieces[0].shape[1]), pieces[0].dtype),
        compiler_params=pltpu.CompilerParams(vmem_limit_bytes=4 * MIB),
        name="lower",
    )(*pieces)


def product(rows, first, second):
    hidden = jnp.maximum(jnp.dot(rows, first, preferred_element_type=jnp.float32), 0.0)
    return jnp.dot(hidden.astype(jnp.bfloat16), second, preferred_element_type=jnp.float32)


def cost(count, weight):
    flops = 8 * count * weight.shape[1] * weight.shape[2]
    return pl.CostEstimate(flops=flops, bytes_accessed=8 * weight.size, transcendentals=0)


def ffn_kernel(in_a, in_b, out_a, out_b, *refs):
    row_refs, result_refs = refs[: len(refs) // 2], refs[len(refs) // 2 :]
    rows = jnp.concatenate([ref[...] for ref in row_refs], axis=0)
    total = product(rows, in_a[0], out_a[0]) + product(rows, in_b[0], out_b[0])
    total = total.astype(jnp.bfloat16)
    start = 0
    for ref in result_refs:
        ref[...] = total[start : start + ref.shape[0]]
        start += ref.shape[0]


def ffn(pieces, weights):
    return pl.pallas_call(
        ffn_kernel,
        out_shape=[jax.ShapeDtypeStruct(p.shape, jnp.bfloat16) for p in pieces],
        compiler_params=pltpu.CompilerParams(vmem_limit_bytes=FFN_LIMIT * MIB),
        cost_estimate=cost(sum(p.shape[0] for p in pieces), weights[0]),
        name="ffn",
    )(*weights, *pieces)


def mix_kernel(wanted_ref, gating_ref, tokens_ref, *refs):
    piece_refs, back_refs, out_ref = refs[:-3], refs[-3:-1], refs[-1]
    part = piece_refs[0].shape[0] // 2
    returned = jnp.concatenate(
        [ref[:part] for ref in piece_refs] + [ref[...] for ref in back_refs], axis=0
    )
    pick = picks(wanted_ref[...], returned.shape[0])
    arrived = lax.dot_general(
        pick, returned, (((0,), (0,)), ((), ())), preferred_element_type=jnp.float32
    )
    gating = jnp.broadcast_to(gating_ref[...], (8, gating_ref.shape[1])).T[:, :1]
    out_ref[...] = (tokens_ref[...].astype(jnp.float32) + gating * arrived).astype(jnp.bfloat16)


def mix(wanted, gating, tokens, pieces, back):
    return pl.pallas_call(
        mix_kernel,
        out_shape=jax.ShapeDtypeStruct(tokens.shape, jnp.bfloat16),
        compiler_params=pltpu.CompilerParams(vmem_limit_bytes=8 * MIB),
        name="mix",
    )(wanted[None, :], gating[None, :], tokens, *pieces, *back)


def gates(tokens, expert_ids, centroids):
    scores = jnp.dot(tokens, centroids.T, preferred_element_type=jnp.float32)
    columns = jnp.arange(centroids.shape[0], dtype=jnp.int32)
    named = columns[None, :] == expert_ids[:, None]
    return jax.nn.sigmoid(jnp.sum(jnp.where(named, scores, 0.0), axis=1))


def other_core():
    pair = lax.axis_size("grp")
    return [(i, (i + 1) % pair) for i in range(pair)]


def plain(tokens, expert_ids, slot_ids, centroids, w_in, w_out):
    experts, (count_rows, model_width) = centroids.shape[0], tokens.shape
    capacity = 2 * count_rows // experts
    far_in = lax.ppermute(w_in, "grp", other_core())
    far_out = lax.ppermute(w_out, "grp", other_core())
    buffer_rows = expert_ids * capacity + slot_ids
    empty = jnp.zeros((experts * capacity, model_width), jnp.bfloat16)
    outgoing = empty.at[buffer_rows].set(tokens).reshape(experts, capacity, model_width)
    received = lax.all_to_all(outgoing, "ex", split_axis=0, concat_axis=0, tiled=True)
    rows = received.reshape(-1, model_width)
    total = product(rows, w_in[0], w_out[0]) + product(rows, far_in[0], far_out[0])
    result = total.astype(jnp.bfloat16).reshape(received.shape)
    returned = lax.all_to_all(result, "ex", split_axis=0, concat_axis=0, tiled=True)
    arrived = returned.reshape(-1, model_width)[buffer_rows].astype(jnp.float32)
    gating = gates(tokens, expert_ids, centroids)
    return (tokens.astype(jnp.float32) + gating[:, None] * arrived).astype(jnp.bfloat16)


def paired(tokens, expert_ids, slot_ids, centroids, w_in, w_out):
    experts, count_rows = centroids.shape[0], tokens.shape[0]
    capacity = 2 * count_rows // experts
    span = experts // 4

    def travel(pieces, first):
        return [
            lax.ppermute(
                piece,
                ("grp", "ex"),
                [
                    (core * experts + i, core * experts + (i ^ (first + 4 * k + core)))
                    for core in range(2)
                    for i in range(experts)
                ],
            )
            for k, piece in enumerate(pieces)
        ]

    def change_core(rows):
        return lax.ppermute(rows, "grp", other_core())

    offset = expert_ids ^ lax.axis_index("ex")
    give = (offset % 2) ^ lax.axis_index("grp")
    close = 1 - offset // (2 * span)
    cut = span // 2
    late = offset // 2 % 2
    wanted = (((2 * give + late) * 2 + close) * cut + offset // 4 % cut) * capacity + slot_ids
    keep_a, keep_b, give_a, give_b = place(wanted, tokens, [span * capacity] * 4)
    got_a = change_core(give_a)
    got_b = change_core(give_b)
    out_a = pack(keep_a, got_a, capacity)
    out_b = pack(keep_b, got_b, capacity)
    far, near = 2 * span, 0
    far_a = travel(out_a[:cut], far)
    near_a = travel(out_a[cut:], near)
    far_b = travel(out_b[:cut], far + 2)
    near_b = travel(out_b[cut:], near + 2)
    far_in = lax.ppermute(w_in, "grp", other_core())
    far_out = lax.ppermute(w_out, "grp", other_core())
    weights = (w_in, far_in, w_out, far_out)
    done_a = ffn([*far_a, *near_a], weights)
    back_a = travel(done_a[:cut], far)
    back_a += travel(done_a[cut:], near)
    done_b = ffn([*far_b, *near_b], weights)
    back_b = travel(done_b[:cut], far + 2)
    back_b += travel(done_b[cut:], near + 2)
    gave_a = change_core(lower(back_a))
    gave_b = change_core(lower(back_b))
    gating = gates(tokens, expert_ids, centroids)
    return mix(wanted, gating, tokens, [*back_a, *back_b], [gave_a, gave_b])


def solution(mesh):
    experts, pair = mesh.shape["ex"], mesh.shape["grp"]
    in_specs = (
        P(("grp", "ex"), None),
        P(("grp", "ex")),
        P(("grp", "ex")),
        P(),
        P("ex", None, "grp"),
        P("ex", "grp", None),
    )
    out_specs = P(("grp", "ex"), None)

    def step(*args):
        capacity = 2 * args[0].shape[0] // (pair * experts * experts)
        large = pair == 2 and experts % 8 == 0 and capacity % 16 == 0
        body = jax.shard_map(
            paired if large else plain,
            mesh=mesh,
            in_specs=in_specs,
            out_specs=out_specs,
            check_vma=False,
        )
        return body(*args)

    return step
```

```python
import jax
import jax.numpy as jnp
from jax import lax
from jax.experimental import pallas as pl
from jax.experimental.pallas import tpu as pltpu
from jax.sharding import PartitionSpec as P


MIB = 1024 * 1024
COVER = 30_000_000_000
FFN_LIMIT = 12


def picks(wanted, total_rows):
    rows = lax.broadcasted_iota(jnp.int32, (total_rows, wanted.shape[1]), 0)
    return jnp.where(rows == wanted, 1.0, 0.0).astype(jnp.bfloat16)


def place_kernel(wanted_ref, tokens_ref, *refs):
    total = sum(ref.shape[0] for ref in refs)
    placed = jnp.dot(
        picks(wanted_ref[...], total), tokens_ref[...], preferred_element_type=jnp.float32
    ).astype(jnp.bfloat16)
    start = 0
    for ref in refs:
        ref[...] = placed[start : start + ref.shape[0]]
        start += ref.shape[0]


def place(wanted, tokens, sizes):
    return pl.pallas_call(
        place_kernel,
        out_shape=[jax.ShapeDtypeStruct((n, tokens.shape[1]), jnp.bfloat16) for n in sizes],
        compiler_params=pltpu.CompilerParams(vmem_limit_bytes=8 * MIB),
        cost_estimate=pl.CostEstimate(flops=COVER, bytes_accessed=0, transcendentals=0),
        name="place",
    )(wanted[None, :], tokens)


def pack_kernel(keep_ref, got_ref, *refs):
    part = keep_ref.shape[0] // len(refs)
    for k, ref in enumerate(refs):
        ref[:part] = keep_ref[k * part : (k + 1) * part]
        ref[part:] = got_ref[k * part : (k + 1) * part]


def pack(keep, got, part):
    piece = jax.ShapeDtypeStruct((2 * part, keep.shape[1]), keep.dtype)
    return pl.pallas_call(
        pack_kernel,
        out_shape=[piece] * (keep.shape[0] // part),
        compiler_params=pltpu.CompilerParams(vmem_limit_bytes=4 * MIB),
        name="pack",
    )(keep, got)


def lower_kernel(*refs):
    piece_refs, out_ref = refs[:-1], refs[-1]
    part = out_ref.shape[0] // len(piece_refs)
    for k, ref in enumerate(piece_refs):
        out_ref[k * part : (k + 1) * part] = ref[part:]


def lower(pieces):
    rows = len(pieces) * pieces[0].shape[0] // 2
    return pl.pallas_call(
        lower_kernel,
        out_shape=jax.ShapeDtypeStruct((rows, pieces[0].shape[1]), pieces[0].dtype),
        compiler_params=pltpu.CompilerParams(vmem_limit_bytes=4 * MIB),
        name="lower",
    )(*pieces)


def product(rows, first, second):
    hidden = jnp.maximum(jnp.dot(rows, first, preferred_element_type=jnp.float32), 0.0)
    return jnp.dot(hidden.astype(jnp.bfloat16), second, preferred_element_type=jnp.float32)


def cost(count, weight):
    flops = 8 * count * weight.shape[1] * weight.shape[2]
    return pl.CostEstimate(flops=flops, bytes_accessed=8 * weight.size, transcendentals=0)


def ffn_kernel(in_a, in_b, out_a, out_b, *refs):
    row_refs, result_refs = refs[: len(refs) // 2], refs[len(refs) // 2 :]
    rows = jnp.concatenate([ref[...] for ref in row_refs], axis=0)
    total = product(rows, in_a[0], out_a[0]) + product(rows, in_b[0], out_b[0])
    total = total.astype(jnp.bfloat16)
    start = 0
    for ref in result_refs:
        ref[...] = total[start : start + ref.shape[0]]
        start += ref.shape[0]


def half_kernel(in_a, out_a, *refs):
    rows = jnp.concatenate([ref[...] for ref in refs[:-1]], axis=0)
    refs[-1][...] = product(rows, in_a[0], out_a[0])


def ffn_half(pieces, first, second):
    rows = sum(p.shape[0] for p in pieces)
    estimate = cost(rows, first)
    return pl.pallas_call(
        half_kernel,
        out_shape=jax.ShapeDtypeStruct((rows, pieces[0].shape[1]), jnp.float32),
        compiler_params=pltpu.CompilerParams(vmem_limit_bytes=FFN_LIMIT * MIB),
        cost_estimate=estimate,
        name="ffn_half",
    )(first, second, *pieces)


def rest_kernel(in_b, out_b, half_ref, *refs):
    row_refs, result_refs = refs[: len(refs) // 2], refs[len(refs) // 2 :]
    rows = jnp.concatenate([ref[...] for ref in row_refs], axis=0)
    total = (half_ref[...] + product(rows, in_b[0], out_b[0])).astype(jnp.bfloat16)
    start = 0
    for ref in result_refs:
        ref[...] = total[start : start + ref.shape[0]]
        start += ref.shape[0]


def ffn_rest(pieces, first, second, half):
    return pl.pallas_call(
        rest_kernel,
        out_shape=[jax.ShapeDtypeStruct(p.shape, jnp.bfloat16) for p in pieces],
        compiler_params=pltpu.CompilerParams(vmem_limit_bytes=FFN_LIMIT * MIB),
        cost_estimate=cost(half.shape[0], first),
        name="ffn_rest",
    )(first, second, half, *pieces)


def ffn(pieces, weights):
    return pl.pallas_call(
        ffn_kernel,
        out_shape=[jax.ShapeDtypeStruct(p.shape, jnp.bfloat16) for p in pieces],
        compiler_params=pltpu.CompilerParams(vmem_limit_bytes=FFN_LIMIT * MIB),
        cost_estimate=cost(sum(p.shape[0] for p in pieces), weights[0]),
        name="ffn",
    )(*weights, *pieces)


def mix_kernel(wanted_ref, gating_ref, tokens_ref, *refs):
    piece_refs, back_refs, out_ref = refs[:-3], refs[-3:-1], refs[-1]
    part = piece_refs[0].shape[0] // 2
    returned = jnp.concatenate(
        [ref[:part] for ref in piece_refs] + [ref[...] for ref in back_refs], axis=0
    )
    pick = picks(wanted_ref[...], returned.shape[0])
    arrived = lax.dot_general(
        pick, returned, (((0,), (0,)), ((), ())), preferred_element_type=jnp.float32
    )
    gating = jnp.broadcast_to(gating_ref[...], (8, gating_ref.shape[1])).T[:, :1]
    out_ref[...] = (tokens_ref[...].astype(jnp.float32) + gating * arrived).astype(jnp.bfloat16)


def mix(wanted, gating, tokens, pieces, back):
    return pl.pallas_call(
        mix_kernel,
        out_shape=jax.ShapeDtypeStruct(tokens.shape, jnp.bfloat16),
        compiler_params=pltpu.CompilerParams(vmem_limit_bytes=8 * MIB),
        name="mix",
    )(wanted[None, :], gating[None, :], tokens, *pieces, *back)


def gates(tokens, expert_ids, centroids):
    scores = jnp.dot(tokens, centroids.T, preferred_element_type=jnp.float32)
    columns = jnp.arange(centroids.shape[0], dtype=jnp.int32)
    named = columns[None, :] == expert_ids[:, None]
    return jax.nn.sigmoid(jnp.sum(jnp.where(named, scores, 0.0), axis=1))


def other_core():
    pair = lax.axis_size("grp")
    return [(i, (i + 1) % pair) for i in range(pair)]


def plain(tokens, expert_ids, slot_ids, centroids, w_in, w_out):
    experts, (count_rows, model_width) = centroids.shape[0], tokens.shape
    capacity = 2 * count_rows // experts
    far_in = lax.ppermute(w_in, "grp", other_core())
    far_out = lax.ppermute(w_out, "grp", other_core())
    buffer_rows = expert_ids * capacity + slot_ids
    empty = jnp.zeros((experts * capacity, model_width), jnp.bfloat16)
    outgoing = empty.at[buffer_rows].set(tokens).reshape(experts, capacity, model_width)
    received = lax.all_to_all(outgoing, "ex", split_axis=0, concat_axis=0, tiled=True)
    rows = received.reshape(-1, model_width)
    total = product(rows, w_in[0], w_out[0]) + product(rows, far_in[0], far_out[0])
    result = total.astype(jnp.bfloat16).reshape(received.shape)
    returned = lax.all_to_all(result, "ex", split_axis=0, concat_axis=0, tiled=True)
    arrived = returned.reshape(-1, model_width)[buffer_rows].astype(jnp.float32)
    gating = gates(tokens, expert_ids, centroids)
    return (tokens.astype(jnp.float32) + gating[:, None] * arrived).astype(jnp.bfloat16)


def paired(tokens, expert_ids, slot_ids, centroids, w_in, w_out):
    experts, count_rows = centroids.shape[0], tokens.shape[0]
    capacity = 2 * count_rows // experts
    span = experts // 4

    def travel(pieces, first):
        return [
            lax.ppermute(
                piece,
                ("grp", "ex"),
                [
                    (core * experts + i, core * experts + (i ^ (first + 4 * k + 2 * core)))
                    for core in range(2)
                    for i in range(experts)
                ],
            )
            for k, piece in enumerate(pieces)
        ]

    def change_core(rows):
        return lax.ppermute(rows, "grp", other_core())

    offset = expert_ids ^ lax.axis_index("ex")
    give = (offset // 2 % 2) ^ lax.axis_index("grp")
    close = 1 - offset // (2 * span)
    cut = span // 2
    late = offset // 1 % 2
    wanted = (((2 * give + late) * 2 + close) * cut + offset // 4 % 2) * capacity + slot_ids
    keep_a, keep_b, give_a, give_b = place(wanted, tokens, [span * capacity] * 4)
    got_a = change_core(give_a)
    got_b = change_core(give_b)
    out_a = pack(keep_a, got_a, capacity)
    out_b = pack(keep_b, got_b, capacity)
    far, near = 2 * span, 0
    far_a = travel(out_a[:cut], far)
    near_a = travel(out_a[cut:], near)
    far_b = travel(out_b[:cut], far + 1)
    near_b = travel(out_b[cut:], near + 1)
    far_in = lax.ppermute(w_in, "grp", other_core())
    far_out = lax.ppermute(w_out, "grp", other_core())
    weights = (w_in, far_in, w_out, far_out)
    half_a = ffn_half([*far_a, *near_a], w_in, w_out)
    done_a = ffn_rest([*far_a, *near_a], far_in, far_out, half_a)
    back_a = travel(done_a[:cut], far)
    back_a += travel(done_a[cut:], near)
    done_b = ffn([*far_b, *near_b], weights)
    back_b = travel(done_b[:cut], far + 1)
    back_b += travel(done_b[cut:], near + 1)
    gave_a = change_core(lower(back_a))
    gave_b = change_core(lower(back_b))
    gating = gates(tokens, expert_ids, centroids)
    return mix(wanted, gating, tokens, [*back_a, *back_b], [gave_a, gave_b])


def solution(mesh):
    experts, pair = mesh.shape["ex"], mesh.shape["grp"]
    in_specs = (
        P(("grp", "ex"), None),
        P(("grp", "ex")),
        P(("grp", "ex")),
        P(),
        P("ex", None, "grp"),
        P("ex", "grp", None),
    )
    out_specs = P(("grp", "ex"), None)

    def step(*args):
        capacity = 2 * args[0].shape[0] // (pair * experts * experts)
        large = pair == 2 and experts % 8 == 0 and capacity % 16 == 0
        body = jax.shard_map(
            paired if large else plain,
            mesh=mesh,
            in_specs=in_specs,
            out_specs=out_specs,
            check_vma=False,
        )
        return body(*args)

    return step
```

```python
import jax
import jax.numpy as jnp
from jax import lax
from jax.experimental import pallas as pl
from jax.experimental.pallas import tpu as pltpu
from jax.sharding import PartitionSpec as P


MIB = 1024 * 1024
COVER = 30_000_000_000
FFN_LIMIT = 12


def picks(wanted, total_rows):
    rows = lax.broadcasted_iota(jnp.int32, (total_rows, wanted.shape[1]), 0)
    return jnp.where(rows == wanted, 1.0, 0.0).astype(jnp.bfloat16)


def place_kernel(wanted_ref, tokens_ref, *refs):
    total = sum(ref.shape[0] for ref in refs)
    placed = jnp.dot(
        picks(wanted_ref[...], total), tokens_ref[...], preferred_element_type=jnp.float32
    ).astype(jnp.bfloat16)
    start = 0
    for ref in refs:
        ref[...] = placed[start : start + ref.shape[0]]
        start += ref.shape[0]


def place(wanted, tokens, sizes):
    return pl.pallas_call(
        place_kernel,
        out_shape=[jax.ShapeDtypeStruct((n, tokens.shape[1]), jnp.bfloat16) for n in sizes],
        compiler_params=pltpu.CompilerParams(vmem_limit_bytes=8 * MIB),
        cost_estimate=pl.CostEstimate(flops=COVER, bytes_accessed=0, transcendentals=0),
        name="place",
    )(wanted[None, :], tokens)


def pack_kernel(keep_ref, got_ref, *refs):
    part = keep_ref.shape[0] // len(refs)
    for k, ref in enumerate(refs):
        ref[:part] = keep_ref[k * part : (k + 1) * part]
        ref[part:] = got_ref[k * part : (k + 1) * part]


def pack(keep, got, part):
    piece = jax.ShapeDtypeStruct((2 * part, keep.shape[1]), keep.dtype)
    return pl.pallas_call(
        pack_kernel,
        out_shape=[piece] * (keep.shape[0] // part),
        compiler_params=pltpu.CompilerParams(vmem_limit_bytes=4 * MIB),
        name="pack",
    )(keep, got)


def lower_kernel(*refs):
    piece_refs, out_ref = refs[:-1], refs[-1]
    part = out_ref.shape[0] // len(piece_refs)
    for k, ref in enumerate(piece_refs):
        out_ref[k * part : (k + 1) * part] = ref[part:]


def lower(pieces):
    rows = len(pieces) * pieces[0].shape[0] // 2
    return pl.pallas_call(
        lower_kernel,
        out_shape=jax.ShapeDtypeStruct((rows, pieces[0].shape[1]), pieces[0].dtype),
        compiler_params=pltpu.CompilerParams(vmem_limit_bytes=4 * MIB),
        name="lower",
    )(*pieces)


def product(rows, first, second):
    hidden = jnp.maximum(jnp.dot(rows, first, preferred_element_type=jnp.float32), 0.0)
    return jnp.dot(hidden.astype(jnp.bfloat16), second, preferred_element_type=jnp.float32)


def cost(count, weight):
    flops = 8 * count * weight.shape[1] * weight.shape[2]
    return pl.CostEstimate(flops=flops, bytes_accessed=8 * weight.size, transcendentals=0)


def ffn_kernel(in_a, in_b, out_a, out_b, *refs):
    row_refs, result_refs = refs[: len(refs) // 2], refs[len(refs) // 2 :]
    rows = jnp.concatenate([ref[...] for ref in row_refs], axis=0)
    total = product(rows, in_a[0], out_a[0]) + product(rows, in_b[0], out_b[0])
    total = total.astype(jnp.bfloat16)
    start = 0
    for ref in result_refs:
        ref[...] = total[start : start + ref.shape[0]]
        start += ref.shape[0]


def half_kernel(in_a, out_a, *refs):
    rows = jnp.concatenate([ref[...] for ref in refs[:-1]], axis=0)
    refs[-1][...] = product(rows, in_a[0], out_a[0])


def ffn_half(pieces, first, second):
    rows = sum(p.shape[0] for p in pieces)
    estimate = cost(rows, first)
    return pl.pallas_call(
        half_kernel,
        out_shape=jax.ShapeDtypeStruct((rows, pieces[0].shape[1]), jnp.float32),
        compiler_params=pltpu.CompilerParams(vmem_limit_bytes=FFN_LIMIT * MIB),
        cost_estimate=estimate,
        name="ffn_half",
    )(first, second, *pieces)


def rest_kernel(in_b, out_b, half_ref, *refs):
    row_refs, result_refs = refs[: len(refs) // 2], refs[len(refs) // 2 :]
    rows = jnp.concatenate([ref[...] for ref in row_refs], axis=0)
    total = (half_ref[...] + product(rows, in_b[0], out_b[0])).astype(jnp.bfloat16)
    start = 0
    for ref in result_refs:
        ref[...] = total[start : start + ref.shape[0]]
        start += ref.shape[0]


def ffn_rest(pieces, first, second, half):
    return pl.pallas_call(
        rest_kernel,
        out_shape=[jax.ShapeDtypeStruct(p.shape, jnp.bfloat16) for p in pieces],
        compiler_params=pltpu.CompilerParams(vmem_limit_bytes=FFN_LIMIT * MIB),
        cost_estimate=cost(half.shape[0], first),
        name="ffn_rest",
    )(first, second, half, *pieces)


def ffn(pieces, weights):
    return pl.pallas_call(
        ffn_kernel,
        out_shape=[jax.ShapeDtypeStruct(p.shape, jnp.bfloat16) for p in pieces],
        compiler_params=pltpu.CompilerParams(vmem_limit_bytes=FFN_LIMIT * MIB),
        cost_estimate=cost(sum(p.shape[0] for p in pieces), weights[0]),
        name="ffn",
    )(*weights, *pieces)


def mix_kernel(wanted_ref, gating_ref, tokens_ref, *refs):
    piece_refs, back_refs, out_ref = refs[:-3], refs[-3:-1], refs[-1]
    part = piece_refs[0].shape[0] // 2
    returned = jnp.concatenate(
        [ref[:part] for ref in piece_refs] + [ref[...] for ref in back_refs], axis=0
    )
    pick = picks(wanted_ref[...], returned.shape[0])
    arrived = lax.dot_general(
        pick, returned, (((0,), (0,)), ((), ())), preferred_element_type=jnp.float32
    )
    gating = jnp.broadcast_to(gating_ref[...], (8, gating_ref.shape[1])).T[:, :1]
    out_ref[...] = (tokens_ref[...].astype(jnp.float32) + gating * arrived).astype(jnp.bfloat16)


def mix(wanted, gating, tokens, pieces, back):
    return pl.pallas_call(
        mix_kernel,
        out_shape=jax.ShapeDtypeStruct(tokens.shape, jnp.bfloat16),
        compiler_params=pltpu.CompilerParams(vmem_limit_bytes=8 * MIB),
        name="mix",
    )(wanted[None, :], gating[None, :], tokens, *pieces, *back)


def gates(tokens, expert_ids, centroids):
    scores = jnp.dot(tokens, centroids.T, preferred_element_type=jnp.float32)
    columns = jnp.arange(centroids.shape[0], dtype=jnp.int32)
    named = columns[None, :] == expert_ids[:, None]
    return jax.nn.sigmoid(jnp.sum(jnp.where(named, scores, 0.0), axis=1))


def other_core():
    pair = lax.axis_size("grp")
    return [(i, (i + 1) % pair) for i in range(pair)]


def plain(tokens, expert_ids, slot_ids, centroids, w_in, w_out):
    experts, (count_rows, model_width) = centroids.shape[0], tokens.shape
    capacity = 2 * count_rows // experts
    far_in = lax.ppermute(w_in, "grp", other_core())
    far_out = lax.ppermute(w_out, "grp", other_core())
    buffer_rows = expert_ids * capacity + slot_ids
    empty = jnp.zeros((experts * capacity, model_width), jnp.bfloat16)
    outgoing = empty.at[buffer_rows].set(tokens).reshape(experts, capacity, model_width)
    received = lax.all_to_all(outgoing, "ex", split_axis=0, concat_axis=0, tiled=True)
    rows = received.reshape(-1, model_width)
    total = product(rows, w_in[0], w_out[0]) + product(rows, far_in[0], far_out[0])
    result = total.astype(jnp.bfloat16).reshape(received.shape)
    returned = lax.all_to_all(result, "ex", split_axis=0, concat_axis=0, tiled=True)
    arrived = returned.reshape(-1, model_width)[buffer_rows].astype(jnp.float32)
    gating = gates(tokens, expert_ids, centroids)
    return (tokens.astype(jnp.float32) + gating[:, None] * arrived).astype(jnp.bfloat16)


def paired(tokens, expert_ids, slot_ids, centroids, w_in, w_out):
    experts, count_rows = centroids.shape[0], tokens.shape[0]
    capacity = 2 * count_rows // experts
    span = experts // 4

    def travel(pieces, first, backwards=False):
        order = list(enumerate(pieces))
        moved = {}
        for k, piece in order[::-1] if backwards else order:
            pairs = [
                (core * experts + i, core * experts + (i ^ (first + 4 * k + 2 * core)))
                for core in range(2)
                for i in range(experts)
            ]
            moved[k] = lax.ppermute(piece, ("grp", "ex"), pairs)
        return [moved[k] for k, _ in order]

    def change_core(rows):
        return lax.ppermute(rows, "grp", other_core())

    offset = expert_ids ^ lax.axis_index("ex")
    give = (offset // 2 % 2) ^ lax.axis_index("grp")
    close = 1 - offset // (2 * span)
    cut = span // 2
    late = offset % 2
    wanted = (((2 * give + late) * 2 + close) * cut + offset // 4 % cut) * capacity + slot_ids
    keep_a, keep_b, give_a, give_b = place(wanted, tokens, [span * capacity] * 4)
    got_a = change_core(give_a)
    got_b = change_core(give_b)
    out_a = pack(keep_a, got_a, capacity)
    out_b = pack(keep_b, got_b, capacity)
    far, near = 2 * span, 0
    far_a = travel(out_a[:cut], far, backwards=True)
    near_a = travel(out_a[cut:], near)
    far_b = travel(out_b[:cut], far + 1)
    near_b = travel(out_b[cut:], near + 1)
    far_in = lax.ppermute(w_in, "grp", other_core())
    far_out = lax.ppermute(w_out, "grp", other_core())
    weights = (w_in, far_in, w_out, far_out)
    half_a = ffn_half([*far_a, *near_a], w_in, w_out)
    done_a = ffn_rest([*far_a, *near_a], far_in, far_out, half_a)
    back_a = travel(done_a[:cut], far)
    back_a += travel(done_a[cut:], near)
    done_b = ffn([*far_b, *near_b], weights)
    back_b = travel(done_b[:cut], far + 1)
    back_b += travel(done_b[cut:], near + 1)
    gave_a = change_core(lower(back_a))
    gave_b = change_core(lower(back_b))
    gating = gates(tokens, expert_ids, centroids)
    return mix(wanted, gating, tokens, [*back_a, *back_b], [gave_a, gave_b])


def solution(mesh):
    experts, pair = mesh.shape["ex"], mesh.shape["grp"]
    in_specs = (
        P(("grp", "ex"), None),
        P(("grp", "ex")),
        P(("grp", "ex")),
        P(),
        P("ex", None, "grp"),
        P("ex", "grp", None),
    )
    out_specs = P(("grp", "ex"), None)

    def step(*args):
        capacity = 2 * args[0].shape[0] // (pair * experts * experts)
        large = pair == 2 and experts % 8 == 0 and experts & (experts - 1) == 0 and capacity % 16 == 0
        body = jax.shard_map(
            paired if large else plain,
            mesh=mesh,
            in_specs=in_specs,
            out_specs=out_specs,
            check_vma=False,
        )
        return body(*args)

    return step
```

```python
import jax
import jax.numpy as jnp
from jax import lax
from jax.experimental import pallas as pl
from jax.experimental.pallas import tpu as pltpu
from jax.sharding import PartitionSpec as P


MIB = 1024 * 1024
COVER = 30_000_000_000
FFN_LIMIT = 12


def picks(wanted, total_rows):
    rows = lax.broadcasted_iota(jnp.int32, (total_rows, wanted.shape[1]), 0)
    return jnp.where(rows == wanted, 1.0, 0.0).astype(jnp.bfloat16)


def place_kernel(wanted_ref, tokens_ref, *refs):
    total = sum(ref.shape[0] for ref in refs)
    placed = jnp.dot(
        picks(wanted_ref[...], total), tokens_ref[...], preferred_element_type=jnp.float32
    ).astype(jnp.bfloat16)
    start = 0
    for ref in refs:
        ref[...] = placed[start : start + ref.shape[0]]
        start += ref.shape[0]


def place(wanted, tokens, sizes):
    return pl.pallas_call(
        place_kernel,
        out_shape=[jax.ShapeDtypeStruct((n, tokens.shape[1]), jnp.bfloat16) for n in sizes],
        compiler_params=pltpu.CompilerParams(vmem_limit_bytes=8 * MIB),
        cost_estimate=pl.CostEstimate(flops=COVER, bytes_accessed=0, transcendentals=0),
        name="place",
    )(wanted[None, :], tokens)


def pack_kernel(keep_ref, got_ref, *refs):
    part = keep_ref.shape[0] // len(refs)
    for k, ref in enumerate(refs):
        ref[:part] = keep_ref[k * part : (k + 1) * part]
        ref[part:] = got_ref[k * part : (k + 1) * part]


def pack(keep, got, part):
    piece = jax.ShapeDtypeStruct((2 * part, keep.shape[1]), keep.dtype)
    return pl.pallas_call(
        pack_kernel,
        out_shape=[piece] * (keep.shape[0] // part),
        compiler_params=pltpu.CompilerParams(vmem_limit_bytes=4 * MIB),
        name="pack",
    )(keep, got)


def lower_kernel(*refs):
    piece_refs, out_ref = refs[:-1], refs[-1]
    part = out_ref.shape[0] // len(piece_refs)
    for k, ref in enumerate(piece_refs):
        out_ref[k * part : (k + 1) * part] = ref[part:]


def lower(pieces):
    rows = len(pieces) * pieces[0].shape[0] // 2
    return pl.pallas_call(
        lower_kernel,
        out_shape=jax.ShapeDtypeStruct((rows, pieces[0].shape[1]), pieces[0].dtype),
        compiler_params=pltpu.CompilerParams(vmem_limit_bytes=4 * MIB),
        name="lower",
    )(*pieces)


def product(rows, first, second):
    hidden = jnp.maximum(jnp.dot(rows, first, preferred_element_type=jnp.float32), 0.0)
    return jnp.dot(hidden.astype(jnp.bfloat16), second, preferred_element_type=jnp.float32)


def cost(count, weight):
    flops = 8 * count * weight.shape[1] * weight.shape[2]
    return pl.CostEstimate(flops=flops, bytes_accessed=8 * weight.size, transcendentals=0)


def ffn_kernel(in_a, in_b, out_a, out_b, *refs):
    row_refs, result_refs = refs[: len(refs) // 2], refs[len(refs) // 2 :]
    rows = jnp.concatenate([ref[...] for ref in row_refs], axis=0)
    total = product(rows, in_a[0], out_a[0]) + product(rows, in_b[0], out_b[0])
    total = total.astype(jnp.bfloat16)
    start = 0
    for ref in result_refs:
        ref[...] = total[start : start + ref.shape[0]]
        start += ref.shape[0]


def half_kernel(in_a, out_a, *refs):
    rows = jnp.concatenate([ref[...] for ref in refs[:-1]], axis=0)
    refs[-1][...] = product(rows, in_a[0], out_a[0])


def ffn_half(pieces, first, second):
    rows = sum(p.shape[0] for p in pieces)
    estimate = cost(rows, first)
    return pl.pallas_call(
        half_kernel,
        out_shape=jax.ShapeDtypeStruct((rows, pieces[0].shape[1]), jnp.float32),
        compiler_params=pltpu.CompilerParams(vmem_limit_bytes=FFN_LIMIT * MIB),
        cost_estimate=estimate,
        name="ffn_half",
    )(first, second, *pieces)


def rest_kernel(in_b, out_b, half_ref, *refs):
    row_refs, result_refs = refs[: len(refs) // 2], refs[len(refs) // 2 :]
    rows = jnp.concatenate([ref[...] for ref in row_refs], axis=0)
    total = (half_ref[...] + product(rows, in_b[0], out_b[0])).astype(jnp.bfloat16)
    start = 0
    for ref in result_refs:
        ref[...] = total[start : start + ref.shape[0]]
        start += ref.shape[0]


def ffn_rest(pieces, first, second, half):
    return pl.pallas_call(
        rest_kernel,
        out_shape=[jax.ShapeDtypeStruct(p.shape, jnp.bfloat16) for p in pieces],
        compiler_params=pltpu.CompilerParams(vmem_limit_bytes=FFN_LIMIT * MIB),
        cost_estimate=cost(half.shape[0], first),
        name="ffn_rest",
    )(first, second, half, *pieces)


def ffn(pieces, weights):
    return pl.pallas_call(
        ffn_kernel,
        out_shape=[jax.ShapeDtypeStruct(p.shape, jnp.bfloat16) for p in pieces],
        compiler_params=pltpu.CompilerParams(vmem_limit_bytes=FFN_LIMIT * MIB),
        cost_estimate=cost(sum(p.shape[0] for p in pieces), weights[0]),
        name="ffn",
    )(*weights, *pieces)


def mix_kernel(wanted_ref, gating_ref, base_ref, *refs):
    piece_refs, back_ref, out_ref = refs[:-2], refs[-2], refs[-1]
    part = piece_refs[0].shape[0] // 2
    returned = jnp.concatenate([ref[:part] for ref in piece_refs] + [back_ref[...]], axis=0)
    pick = picks(wanted_ref[...], returned.shape[0])
    arrived = lax.dot_general(
        pick, returned, (((0,), (0,)), ((), ())), preferred_element_type=jnp.float32
    )
    gating = jnp.broadcast_to(gating_ref[...], (8, gating_ref.shape[1])).T[:, :1]
    total = base_ref[...].astype(jnp.float32) + gating * arrived
    out_ref[...] = total.astype(out_ref.dtype)


def mix(wanted, gating, base, pieces, back, dtype):
    return pl.pallas_call(
        mix_kernel,
        out_shape=jax.ShapeDtypeStruct(base.shape, dtype),
        compiler_params=pltpu.CompilerParams(vmem_limit_bytes=8 * MIB),
        name="mix",
    )(wanted[None, :], gating[None, :], base, *pieces, back)


def gates(tokens, expert_ids, centroids):
    scores = jnp.dot(tokens, centroids.T, preferred_element_type=jnp.float32)
    columns = jnp.arange(centroids.shape[0], dtype=jnp.int32)
    named = columns[None, :] == expert_ids[:, None]
    return jax.nn.sigmoid(jnp.sum(jnp.where(named, scores, 0.0), axis=1))


def other_core():
    pair = lax.axis_size("grp")
    return [(i, (i + 1) % pair) for i in range(pair)]


def plain(tokens, expert_ids, slot_ids, centroids, w_in, w_out):
    experts, (count_rows, model_width) = centroids.shape[0], tokens.shape
    capacity = 2 * count_rows // experts
    far_in = lax.ppermute(w_in, "grp", other_core())
    far_out = lax.ppermute(w_out, "grp", other_core())
    buffer_rows = expert_ids * capacity + slot_ids
    empty = jnp.zeros((experts * capacity, model_width), jnp.bfloat16)
    outgoing = empty.at[buffer_rows].set(tokens).reshape(experts, capacity, model_width)
    received = lax.all_to_all(outgoing, "ex", split_axis=0, concat_axis=0, tiled=True)
    rows = received.reshape(-1, model_width)
    total = product(rows, w_in[0], w_out[0]) + product(rows, far_in[0], far_out[0])
    result = total.astype(jnp.bfloat16).reshape(received.shape)
    returned = lax.all_to_all(result, "ex", split_axis=0, concat_axis=0, tiled=True)
    arrived = returned.reshape(-1, model_width)[buffer_rows].astype(jnp.float32)
    gating = gates(tokens, expert_ids, centroids)
    return (tokens.astype(jnp.float32) + gating[:, None] * arrived).astype(jnp.bfloat16)


def paired(tokens, expert_ids, slot_ids, centroids, w_in, w_out):
    experts, count_rows = centroids.shape[0], tokens.shape[0]
    capacity = 2 * count_rows // experts
    span = experts // 4

    def travel(pieces, first, backwards=False):
        order = list(enumerate(pieces))
        moved = {}
        for k, piece in order[::-1] if backwards else order:
            pairs = [
                (core * experts + i, core * experts + (i ^ (first + 4 * k + 2 * core)))
                for core in range(2)
                for i in range(experts)
            ]
            moved[k] = lax.ppermute(piece, ("grp", "ex"), pairs)
        return [moved[k] for k, _ in order]

    def change_core(rows):
        return lax.ppermute(rows, "grp", other_core())

    offset = expert_ids ^ lax.axis_index("ex")
    give = (offset // 2 % 2) ^ lax.axis_index("grp")
    close = 1 - offset // (2 * span)
    cut = span // 2
    late = offset % 2
    wanted = (((2 * give + late) * 2 + close) * cut + offset // 4 % cut) * capacity + slot_ids
    keep_a, keep_b, give_a, give_b = place(wanted, tokens, [span * capacity] * 4)
    got_a = change_core(give_a)
    got_b = change_core(give_b)
    out_a = pack(keep_a, got_a, capacity)
    out_b = pack(keep_b, got_b, capacity)
    far, near = 2 * span, 0
    far_a = travel(out_a[:cut], far, backwards=True)
    near_a = travel(out_a[cut:], near, backwards=True)
    far_b = travel(out_b[:cut], far + 1)
    near_b = travel(out_b[cut:], near + 1, backwards=True)
    far_in = lax.ppermute(w_in, "grp", other_core())
    far_out = lax.ppermute(w_out, "grp", other_core())
    weights = (w_in, far_in, w_out, far_out)
    half_a = ffn_half([*far_a, *near_a], w_in, w_out)
    done_a = ffn_rest([*far_a, *near_a], far_in, far_out, half_a)
    back_a = travel(done_a[:cut], far)
    back_a += travel(done_a[cut:], near)
    done_b = ffn([*far_b, *near_b], weights)
    back_b = travel(done_b[:cut], far + 1)
    back_b += travel(done_b[cut:], near + 1)
    gave_a = change_core(lower(back_a))
    gave_b = change_core(lower(back_b))
    gating = gates(tokens, expert_ids, centroids)
    row = ((give * 2 + close) * cut + offset // 4 % cut) * capacity + slot_ids
    wanted_a = jnp.where(late == 0, row, -1)
    wanted_b = jnp.where(late == 1, row, -1)
    half_done = mix(wanted_a, gating, tokens, back_a, gave_a, jnp.float32)
    return mix(wanted_b, gating, half_done, back_b, gave_b, jnp.bfloat16)


def solution(mesh):
    experts, pair = mesh.shape["ex"], mesh.shape["grp"]
    in_specs = (
        P(("grp", "ex"), None),
        P(("grp", "ex")),
        P(("grp", "ex")),
        P(),
        P("ex", None, "grp"),
        P("ex", "grp", None),
    )
    out_specs = P(("grp", "ex"), None)

    def step(*args):
        capacity = 2 * args[0].shape[0] // (pair * experts * experts)
        large = pair == 2 and experts % 8 == 0 and experts & (experts - 1) == 0 and capacity % 16 == 0
        body = jax.shard_map(
            paired if large else plain,
            mesh=mesh,
            in_specs=in_specs,
            out_specs=out_specs,
            check_vma=False,
        )
        return body(*args)

    return step
```
